32 devices in a mesh: stage: 2 (over x), data: 16 (over z, y, core).
Axes of the slice: x: 2, y: 2, z: 4, core: 2. Of those that a mesh axis runs over, the one named last changes fastest.
Arguments:
- w_master: float32 [32, 512, 2048], P('stage', 'data'), parts along dimension 0
- momentum: float32 [32, 512, 2048], P('stage', 'data'), parts along dimension 0
- grads: bfloat16 [32, 16, 512, 2048], P(('stage', 'data')), parts along dimension 0
Outputs:
- output 1: float32 [32, 512, 2048], P('stage', 'data'), parts along dimension 0
- output 2: float32 [32, 512, 2048], P('stage', 'data'), parts along dimension 0
There are 2 independent parts. The reference program is written for one: setup_inputs(seed, part) draws one part's arguments, and reference() takes and returns one part's arrays. A program takes and returns all parts, laid end to end along the dimension named above; each array names one.
All inputs are finite; a program needn't handle non-finite values.
Results may differ from the reference program's by a relative error of at most 0.0109877.
Values are sent between devices in bfloat16 or wider.
A program may use at most 1 GiB of HBM per device.

```python
import math
import jax
import jax.numpy as jnp
from jax import lax

GROUP_SIZE = 16
NUM_MATS = 16
MAT_ROWS = 512
MAT_COLS = 2048
NS_ITERS = 5

MOMENTUM_COEF = 0.95
LEARN_RATE = 0.05
WEIGHT_DECAY = 0.2
NORM_EPS = 1e-7
COEF_A = 3.4445
COEF_B = -4.7750
COEF_C = 2.0315
RMS_SCALE = 0.2 * math.sqrt(max(MAT_ROWS, MAT_COLS))


def setup_inputs(seed: int = 0, part: int = 0) -> dict:
    base_key = jax.random.fold_in(jax.random.key(seed), part)
    sub_keys = jax.random.split(base_key, 6)
    mat_shape = (NUM_MATS, MAT_ROWS, MAT_COLS)
    w_master = 0.02 * jax.random.normal(sub_keys[0], mat_shape, jnp.float32)
    noise_base = jax.random.normal(sub_keys[1], mat_shape, jnp.float32)
    low_left = jax.random.normal(sub_keys[2], (NUM_MATS, MAT_ROWS, 4), jnp.float32)
    low_right = jax.random.normal(sub_keys[3], (NUM_MATS, 4, MAT_COLS), jnp.float32)
    shared = 0.25 * jnp.einsum('mrk,mkc->mrc', low_left, low_right)
    row_scale = jax.random.uniform(sub_keys[4], (NUM_MATS, MAT_ROWS, 1), jnp.float32, 0.5, 1.5)
    momentum = row_scale * (noise_base + shared)
    grads = (jax.random.normal(sub_keys[5], (GROUP_SIZE,) + mat_shape, jnp.float32) * GROUP_SIZE ** -0.5).astype(jnp.bfloat16)
    return {'w_master': w_master, 'momentum': momentum, 'grads': grads}


def newton_schulz(x_start):
    is_tall = MAT_ROWS > MAT_COLS
    x_cur = x_start.T if is_tall else x_start
    for _ in range(NS_ITERS):
        gram_mat = jnp.dot(x_cur, x_cur.T, preferred_element_type=jnp.float32).astype(jnp.bfloat16)
        gram_sq = jnp.dot(gram_mat, gram_mat, preferred_element_type=jnp.float32)
        poly_mat = (COEF_B * gram_mat.astype(jnp.float32) + COEF_C * gram_sq).astype(jnp.bfloat16)
        poly_x = jnp.dot(poly_mat, x_cur, preferred_element_type=jnp.float32)
        x_cur = (COEF_A * x_cur.astype(jnp.float32) + poly_x).astype(jnp.bfloat16)
    return x_cur.T if is_tall else x_cur


def reference(w_master, momentum, grads):
    grad_sum = jnp.sum(grads.astype(jnp.float32), axis=0)
    mom_new = MOMENTUM_COEF * momentum + grad_sum
    frob_norm = jnp.sqrt(jnp.sum(mom_new * mom_new, axis=(1, 2)))

    def one_matrix(mat_pair):
        mom_one, norm_one = mat_pair
        x_start = (mom_one.astype(jnp.bfloat16).astype(jnp.float32) / (norm_one + NORM_EPS)).astype(jnp.bfloat16)
        return newton_schulz(x_start)

    x_ortho = lax.map(one_matrix, (mom_new, frob_norm))
    w_new = w_master - LEARN_RATE * (x_ortho.astype(jnp.float32) * RMS_SCALE + WEIGHT_DECAY * w_master)
    return w_new, mom_new
```

```python
import functools
import math
import jax
import jax.numpy as jnp
from jax import lax
from jax.experimental import pallas as pl
from jax.experimental.pallas import tpu as pltpu
from jax.sharding import PartitionSpec as P

MOMENTUM_COEF = 0.95
LEARN_RATE = 0.05
WEIGHT_DECAY = 0.2
NORM_EPS = 1e-7
COEF_A = 3.4445
COEF_B = -4.7750
COEF_C = 2.0315
NS_ITERS = 5

NZ, NY_, NC = 4, 2, 2
ROWS_B = 16
COLS_Z_FIRST = 256
LAG_Y = 1
LAG_R = 3
HOP = 2
LAG_X = 2
LAG_W = 4

N_P = 2 * LAG_Y + 2
N_S = 3
N_R = 2 * LAG_R + 3 * HOP + 3 - 2 * LAG_Y
N_H = 4 * HOP + 3
N_X = 4


def muon_kernel(n_mats, rows, cols, split, g_hbm, mom_hbm, w_hbm, mom_out, w_out,
                own, prt, ysend, tsum, yrecv, upr, dnr, tsb, upb, dnb, frv,
                momv, wv, xs, xv, ov, gram, poly, ssq_part, ssq_all,
                own_sem, p_ssem, p_rsem, y_ssem, y_rsem, u_ssem, u_rsem, d_ssem, d_rsem,
                ub_ssem, ub_rsem, db_ssem, db_rsem, f_ssem, f_rsem,
                x_ssem, x_rsem, q_ssem, q_rsem, o_ssem, o_rsem, l_sem, mo_sem, wo_sem):
    stage = lax.axis_index('stage')
    me = lax.axis_index('data')
    n_dev = NZ * NY_ * NC
    z = me // 4
    y = (me // 2) % 2
    c = me % 2
    per_mat = rows // ROWS_B
    chunks = n_mats * per_mat
    n_rows = rows * n_dev
    mine = ((3 * z) % 4) * 4 + me % 4
    rms_scale = 0.2 * math.sqrt(max(n_rows, cols))
    lag_z0 = LAG_R
    lag_f = LAG_R + 3 * HOP
    lag_bf = LAG_Y + 3 * HOP
    lag_w = lag_f + LAG_X + NS_ITERS + LAG_W

    def owner(m):
        return ((3 * (m // 4)) % 4) * 4 + m % 4

    def remote(src, dst, ssem, rsem, dev):
        return pltpu.make_async_remote_copy(
            src_ref=src, dst_ref=dst, send_sem=ssem, recv_sem=rsem,
            device_id=(stage, dev), device_id_type=pl.DeviceIdType.MESH)

    partner = z * 4 + y * 2 + (1 - c)
    ynbr = z * 4 + (1 - y) * 2 + c

    def g_slice(k, core):
        return g_hbm.at[k // per_mat, :, :, core, pl.ds((k % per_mat) * ROWS_B, ROWS_B), :]

    def own_copy(k):
        return pltpu.make_async_copy(g_slice(k, c), own.at[k % N_P], own_sem.at[k % N_P])

    def prt_copy(k):
        return remote(g_slice(k, 1 - c), prt.at[k % N_P], p_ssem.at[k % N_P], p_rsem.at[k % N_P], partner)

    def y_copy(k):
        return remote(ysend.at[k % N_S], yrecv.at[k % N_R], y_ssem.at[k % N_S], y_rsem.at[k % N_R], ynbr)

    def up_copy(k, zp):
        return remote(tsum.at[k % N_R, zp], upr.at[k % N_H, zp], u_ssem.at[k % N_R, zp], u_rsem.at[k % N_H, zp], me + 4)

    def dn_copy(k, zp):
        return remote(tsum.at[k % N_R, zp], dnr.at[k % N_H, zp], d_ssem.at[k % N_R, zp], d_rsem.at[k % N_H, zp], me - 4)

    def upb_copy(k, zp):
        return remote(tsb.at[k % N_R, zp], upb.at[k % N_H, zp], ub_ssem.at[k % N_R, zp], ub_rsem.at[k % N_H, zp], me + 4)

    def dnb_copy(k, zp):
        return remote(tsb.at[k % N_R, zp], dnb.at[k % N_H, zp], db_ssem.at[k % N_R, zp], db_rsem.at[k % N_H, zp], me - 4)

    def f_copy(k):
        return remote(tsb.at[k % N_R, z, 1 - y], frv.at[k % N_R], f_ssem.at[k % N_R], f_rsem.at[k % N_R], ynbr)

    def x_copy(k):
        m = k // per_mat
        r0 = (k % per_mat) * ROWS_B
        return remote(xs.at[k % N_X], xv.at[pl.ds(me * rows + r0, ROWS_B), :], x_ssem.at[k % N_X], x_rsem, owner(m))

    def q_copy(m):
        return remote(ssq_part.at[m], ssq_all.at[me], q_ssem, q_rsem, owner(m))

    def o_copy(dev):
        return remote(xv.at[pl.ds(dev * rows, rows), :], ov.at[mine], o_ssem, o_rsem.at[mine], dev)

    def mo_copy(k):
        m = k // per_mat
        rs = pl.ds((k % per_mat) * ROWS_B, ROWS_B)
        return pltpu.make_async_copy(momv.at[m, rs, :], mom_out.at[m, rs, :], mo_sem)

    mom_in = pltpu.make_async_copy(mom_hbm, momv, l_sem.at[0])
    w_in = pltpu.make_async_copy(w_hbm, wv, l_sem.at[1])

    barrier = pltpu.get_barrier_semaphore()

    def greet(i, carry):
        pl.semaphore_signal(barrier, inc=1, device_id=(stage, (me + i) % n_dev), device_id_type=pl.DeviceIdType.MESH)
        return carry

    lax.fori_loop(1, n_dev, greet, 0)

    @pl.when(z == 0)
    def _():
        upr[...] = jnp.zeros_like(upr)
        upb[...] = jnp.zeros_like(upb)

    @pl.when(z == NZ - 1)
    def _():
        dnr[...] = jnp.zeros_like(dnr)
        dnb[...] = jnp.zeros_like(dnb)

    pl.semaphore_wait(barrier, n_dev - 1)

    def at(k, lo=0, hi=chunks):
        return jnp.logical_and(k >= lo, k < hi)

    def step(s, carry):
        @pl.when(s < chunks)
        def _():
            own_copy(s).start()
            prt_copy(s).start()

        @pl.when(s == 1)
        def _():
            mom_in.start()

        @pl.when(s == 4)
        def _():
            w_in.start()

        ky = s - LAG_Y

        @pl.when(at(ky, N_S, chunks + N_S))
        def _():
            y_copy(ky - N_S).wait_send()

        @pl.when(at(ky, N_R, chunks + N_R))
        def _():
            for zp in range(NZ):
                @pl.when(zp > z)
                def _():
                    up_copy(ky - N_R, zp).wait_send()
                    upb_copy(ky - N_R, zp).wait_send()

                @pl.when(zp < z)
                def _():
                    dn_copy(ky - N_R, zp).wait_send()
                    dnb_copy(ky - N_R, zp).wait_send()
            f_copy(ky - N_R).wait_send()

        @pl.when(at(ky))
        def _():
            own_copy(ky).wait()
            prt_copy(ky).wait_send()
            prt_copy(ky).wait_recv()
            ip, it = ky % N_P, ky % N_R

            def other(zp, carry):
                ysend[ky % N_S, zp] = (own[ip, zp, 1 - y, :, :split].astype(jnp.float32)
                                       + prt[ip, zp, 1 - y, :, :split].astype(jnp.float32))
                return carry

            def same(zp, carry):
                tsum[it, zp] = (own[ip, zp, y, :, :split].astype(jnp.float32)
                                + prt[ip, zp, y, :, :split].astype(jnp.float32))
                for yp in range(NY_):
                    tsb[it, zp, yp] = (own[ip, zp, yp, :, split:].astype(jnp.float32)
                                       + prt[ip, zp, yp, :, split:].astype(jnp.float32))
                return carry

            lax.fori_loop(0, NZ, other, 0)
            lax.fori_loop(0, NZ, same, 0)
            y_copy(ky).start()

        kbu = s - LAG_Y - HOP * z

        @pl.when(at(kbu))
        def _():
            for zp in range(1, NZ):
                @pl.when(zp > z)
                def _():
                    @pl.when(z > 0)
                    def _():
                        upb_copy(kbu, zp).wait_recv()
                    tsb[kbu % N_R, zp] += upb[kbu % N_H, zp]
            for zp in range(NZ - 1, 0, -1):
                @pl.when(zp > z)
                def _():
                    upb_copy(kbu, zp).start()

        kbd = s - LAG_Y - HOP * (NZ - 1 - z)

        @pl.when(at(kbd))
        def _():
            for zp in range(NZ - 1):
                @pl.when(zp < z)
                def _():
                    @pl.when(z < NZ - 1)
                    def _():
                        dnb_copy(kbd, zp).wait_recv()
                    tsb[kbd % N_R, zp] += dnb[kbd % N_H, zp]
            for zp in range(NZ - 1):
                @pl.when(zp < z)
                def _():
                    dnb_copy(kbd, zp).start()

        kbf = s - lag_bf

        @pl.when(at(kbf))
        def _():
            @pl.when(z > 0)
            def _():
                upb_copy(kbf, z).wait_recv()

            @pl.when(z < NZ - 1)
            def _():
                dnb_copy(kbf, z).wait_recv()
            tsb[kbf % N_R, z] += upb[kbf % N_H, z] + dnb[kbf % N_H, z]
            f_copy(kbf).start()

        kr = s - LAG_R

        @pl.when(at(kr))
        def _():
            y_copy(kr).wait_recv()

        ku = s - lag_z0 - HOP * z

        @pl.when(at(ku))
        def _():
            for zp in range(NZ - 1, 0, -1):
                @pl.when(zp > z)
                def _():
                    @pl.when(z > 0)
                    def _():
                        up_copy(ku, zp).wait_recv()
                    tsum[ku % N_R, zp] += yrecv[ku % N_R, zp] + upr[ku % N_H, zp]
            for zp in range(NZ - 1, 0, -1):
                @pl.when(zp > z)
                def _():
                    up_copy(ku, zp).start()

        kd = s - lag_z0 - HOP * (NZ - 1 - z)

        @pl.when(at(kd))
        def _():
            for zp in range(NZ - 1):
                @pl.when(zp < z)
                def _():
                    @pl.when(z < NZ - 1)
                    def _():
                        dn_copy(kd, zp).wait_recv()
                    tsum[kd % N_R, zp] += yrecv[kd % N_R, zp] + dnr[kd % N_H, zp]
            for zp in range(NZ - 1):
                @pl.when(zp < z)
                def _():
                    dn_copy(kd, zp).start()

        kf = s - lag_f

        @pl.when(kf == 0)
        def _():
            mom_in.wait()
            ssq_part[...] = jnp.zeros_like(ssq_part)

        @pl.when(at(kf, N_X, chunks + N_X))
        def _():
            kx = kf - N_X

            @pl.when(owner(kx // per_mat) != me)
            def _():
                x_copy(kx).wait_send()

        @pl.when(at(kf))
        def _():
            @pl.when(z > 0)
            def _():
                up_copy(kf, z).wait_recv()

            @pl.when(z < NZ - 1)
            def _():
                dn_copy(kf, z).wait_recv()
            f_copy(kf).wait_recv()
            m = kf // per_mat
            r0 = pl.multiple_of((kf % per_mat) * ROWS_B, ROWS_B)
            it, ih = kf % N_R, kf % N_H
            g_a = (tsum[it, z] + yrecv[it, z]) + (upr[ih, z] + dnr[ih, z])
            m_a = MOMENTUM_COEF * momv[m, pl.ds(r0, ROWS_B), :split] + g_a
            momv[m, pl.ds(r0, ROWS_B), :split] = m_a
            xs[kf % N_X, :, :split] = m_a.astype(jnp.bfloat16)
            g_b = tsb[it, z, y] + frv[it]
            m_b = MOMENTUM_COEF * momv[m, pl.ds(r0, ROWS_B), split:] + g_b
            momv[m, pl.ds(r0, ROWS_B), split:] = m_b
            xs[kf % N_X, :, split:] = m_b.astype(jnp.bfloat16)
            sq_a, sq_b = m_a * m_a, m_b * m_b
            part = ssq_part[m]
            for r in range(0, ROWS_B, 8):
                for j in range(0, split, 128):
                    part = part + sq_a[r:r + 8, j:j + 128]
                for j in range(0, cols - split, 128):
                    part = part + sq_b[r:r + 8, j:j + 128]
            ssq_part[m] = part
            mo_copy(kf).start()
            last = kf % per_mat == per_mat - 1

            @pl.when(owner(m) == me)
            def _():
                xv[pl.ds(pl.multiple_of(me * rows + r0, ROWS_B), ROWS_B), :] = xs[kf % N_X]

                @pl.when(last)
                def _():
                    ssq_all[me] = ssq_part[m]

            @pl.when(owner(m) != me)
            def _():
                x_copy(kf).start()

                @pl.when(last)
                def _():
                    q_copy(m).start()

        q = s - ((mine + 1) * per_mat - 1 + lag_f + LAG_X)

        @pl.when(q == 0)
        def _():
            others = pl.ds(0, (n_dev - 1) * rows)
            pltpu.make_async_copy(xv.at[others, :], xv.at[others, :], x_rsem).wait()
            parts = pl.ds(0, n_dev - 1)
            pltpu.make_async_copy(ssq_all.at[parts], ssq_all.at[parts], q_rsem).wait()
            nrm = jnp.sqrt(jnp.sum(jnp.sum(ssq_all[...], axis=0), keepdims=True))
            inv = 1.0 / (nrm + NORM_EPS)

            def scale(i, carry):
                rs = pl.ds(pl.multiple_of(i * 32, 32), 32)
                xv[rs, :] = (xv[rs, :].astype(jnp.float32) * inv).astype(jnp.bfloat16)
                return carry

            lax.fori_loop(0, n_rows // 32, scale, 0)

        @pl.when(at(q, 1, NS_ITERS + 1))
        def _():
            tile = 256

            def gram_tile(j, carry):
                js = pl.ds(pl.multiple_of(j * tile, tile), tile)
                gram[:, js] = lax.dot_general(
                    xv[...], xv[js, :], (((1,), (1,)), ((), ())),
                    preferred_element_type=jnp.float32).astype(jnp.bfloat16)
                return carry

            def poly_tile(j, carry):
                js = pl.ds(pl.multiple_of(j * tile, tile), tile)
                sq = jnp.dot(gram[...], gram[:, js], preferred_element_type=jnp.float32)
                poly[:, js] = (COEF_B * gram[:, js].astype(jnp.float32) + COEF_C * sq).astype(jnp.bfloat16)
                return carry

            def x_tile(j, carry):
                js = pl.ds(pl.multiple_of(j * tile, tile), tile)
                px = jnp.dot(poly[...], xv[:, js], preferred_element_type=jnp.float32)
                xv[:, js] = (COEF_A * xv[:, js].astype(jnp.float32) + px).astype(jnp.bfloat16)
                return carry

            lax.fori_loop(0, n_rows // tile, gram_tile, 0)
            lax.fori_loop(0, n_rows // tile, poly_tile, 0)
            lax.fori_loop(0, cols // tile, x_tile, 0)

        @pl.when(q == NS_ITERS)
        def _():
            def give(i, carry):
                o_copy((me + i) % n_dev).start()
                return carry

            lax.fori_loop(1, n_dev, give, 0)
            ov[mine] = xv[pl.ds(pl.multiple_of(me * rows, rows), rows), :]

        kw = s - lag_w

        @pl.when(kw == 0)
        def _():
            w_in.wait()

        @pl.when(jnp.logical_and(at(kw), kw % per_mat == per_mat - 1))
        def _():
            m = kw // per_mat

            @pl.when(owner(m) != me)
            def _():
                remote(ov.at[m], ov.at[m], o_ssem, o_rsem.at[m], me).wait_recv()

            w = wv[m]
            wv[m] = w - LEARN_RATE * (ov[m].astype(jnp.float32) * rms_scale + WEIGHT_DECAY * w)
            pltpu.make_async_copy(wv.at[m], w_out.at[m], wo_sem).start()

        return carry

    lax.fori_loop(0, chunks + lag_w, step, 0)
    pltpu.make_async_copy(momv, mom_out, mo_sem).wait()
    pltpu.make_async_copy(wv, w_out, wo_sem).wait()
    others = pl.ds(0, (n_dev - 1) * rows)
    pltpu.make_async_copy(xv.at[others, :], xv.at[others, :], o_ssem).wait()
    sent = pl.ds(0, n_mats - 1)
    pltpu.make_async_copy(ssq_part.at[sent], ssq_part.at[sent], q_ssem).wait()


def solution(mesh):
    row_spec = P('stage', 'data', None)
    grad_spec = P(('stage', 'data'), None, None, None)
    f32, bf16 = jnp.float32, jnp.bfloat16

    def local_step(w_rows, mom_rows, grad_full):
        n_mats, rows, cols = w_rows.shape
        n_rows = grad_full.shape[2]
        split = cols - COLS_Z_FIRST
        g = grad_full.reshape(n_mats, NZ, NY_, NC, rows, cols)
        rb, cb = ROWS_B, COLS_Z_FIRST
        dma = pltpu.SemaphoreType.DMA
        scratch = [
            pltpu.VMEM((N_P, NZ, NY_, rb, cols), bf16),
            pltpu.VMEM((N_P, NZ, NY_, rb, cols), bf16),
            pltpu.VMEM((N_S, NZ, rb, split), f32),
            pltpu.VMEM((N_R, NZ, rb, split), f32),
            pltpu.VMEM((N_R, NZ, rb, split), f32),
            pltpu.VMEM((N_H, NZ, rb, split), f32),
            pltpu.VMEM((N_H, NZ, rb, split), f32),
            pltpu.VMEM((N_R, NZ, NY_, rb, cb), f32),
            pltpu.VMEM((N_H, NZ, NY_, rb, cb), f32),
            pltpu.VMEM((N_H, NZ, NY_, rb, cb), f32),
            pltpu.VMEM((N_R, rb, cb), f32),
            pltpu.VMEM((n_mats, rows, cols), f32),
            pltpu.VMEM((n_mats, rows, cols), f32),
            pltpu.VMEM((N_X, rb, cols), bf16),
            pltpu.VMEM((n_rows, cols), bf16),
            pltpu.VMEM((n_mats, rows, cols), bf16),
            pltpu.VMEM((n_rows, n_rows), bf16),
            pltpu.VMEM((n_rows, n_rows), bf16),
            pltpu.VMEM((n_mats, 8, 128), f32),
            pltpu.VMEM((NZ * NY_ * NC, 8, 128), f32),
            dma((N_P,)), dma((N_P,)), dma((N_P,)), dma((N_S,)), dma((N_R,)),
            dma((N_R, NZ)), dma((N_H, NZ)), dma((N_R, NZ)), dma((N_H, NZ)),
            dma((N_R, NZ)), dma((N_H, NZ)), dma((N_R, NZ)), dma((N_H, NZ)),
            dma((N_R,)), dma((N_R,)),
            dma((N_X,)), dma(()), dma(()), dma(()), dma(()), dma((n_mats,)),
            dma((2,)), dma(()), dma(()),
        ]
        hbm = pl.BlockSpec(memory_space=pltpu.HBM)
        mom_new, w_new = pl.pallas_call(
            functools.partial(muon_kernel, n_mats, rows, cols, split),
            out_shape=[jax.ShapeDtypeStruct(w_rows.shape, f32)] * 2,
            in_specs=[hbm] * 3,
            out_specs=[hbm] * 2,
            scratch_shapes=scratch,
            compiler_params=pltpu.CompilerParams(
                collective_id=0, has_side_effects=True, vmem_limit_bytes=60 * 1024 * 1024),
            name='muon',
        )(g, mom_rows, w_rows)
        return w_new, mom_new

    return jax.shard_map(local_step, mesh=mesh, in_specs=(row_spec, row_spec, grad_spec), out_specs=(row_spec, row_spec), check_vma=False)
```
